32 devices in a mesh: dp: 32 (over z, y, x, core).
Axes of the slice: x: 2, y: 2, z: 4, core: 2. Of those that a mesh axis runs over, the one named last changes fastest.
Arguments:
- features: bfloat16 [32768, 3136], P('dp'), may hold values from -6 to 6
- w_one: bfloat16 [512, 3136], replicated, may hold values from -0.109375 to 0.109375
- b_one: float32 [512], replicated, may hold values from -3 to 3
- w_two: bfloat16 [512, 918], replicated, may hold values from -0.25 to 0.25
- b_two: float32 [918], replicated, may hold values from -112 to 112
- action: int32 [32768], P('dp'), may hold values from 0 to 17
- target_probs: float32 [32768, 18, 51], P('dp'), may hold values from 0 to 1, as said below
- next_action: int32 [32768], P('dp'), may hold values from 0 to 17
- lower_idx: int32 [32768, 51], P('dp'), may hold values from 0 to 49
- upper_frac: float32 [32768, 51], P('dp'), may hold values from 0 to 1
- is_weight: float32 [32768], P('dp'), may hold values from 0.1 to 1
Outputs:
- grad_w1: float32 [512, 3136], replicated
- grad_b1: float32 [512], replicated
- grad_w2: float32 [512, 918], replicated
- grad_b2: float32 [918], replicated
- mean_loss: float32 [], replicated
- priorities: float32 [32768], P('dp')
The draws below stay inside these ranges and needn't reach their ends.
Inputs may be any that keep to these rules, and one draw needn't show every extreme that they name: Each target_probs[i, a] is a distribution over the atoms: positive entries that sum to one.
All inputs are finite; a program needn't handle non-finite values.
Results may differ from the reference program's by a relative error of at most 0.005.
Values sent between devices are 32-bit elements; how exact they have to be, the bound alone decides.
A program may use at most 128 MiB of HBM per device.

```python
import math
import jax
import jax.numpy as jnp
from jax import lax

FEAT = 3136
HID = 512
ACTIONS = 18
ATOMS = 51
ROWS = 1024
TOTAL = 32768
N_DP = 32


def draw_b_two(key, part):
    key_noise, key_shift, key_order = jax.random.split(key, 3)
    return jnp.clip(0.5 * jax.random.normal(key_noise, (ACTIONS * ATOMS,), jnp.float32), -2.0, 2.0)


def draw_target_probs(key, part):
    key_main, key_scale = jax.random.split(key, 2)
    scores = 1.5 * jax.random.normal(key_main, (TOTAL, ACTIONS, ATOMS), jnp.float32)
    return jax.nn.softmax(scores, axis=-1)


def with_ends(values, key, low, top_value):
    spot = [jax.random.randint(jax.random.fold_in(key, axis), (), 0, length) for axis, length in enumerate(values.shape)]
    widest = values.shape.index(max(values.shape))
    beside = spot[:widest] + [(spot[widest] + 1) % values.shape[widest]] + spot[widest + 1:]
    return values.at[tuple(spot)].set(low).at[tuple(beside)].set(top_value)


def levels(key, dims, pieces, smallest, high):
    def one(dim, parts):
        heights = jax.random.uniform(jax.random.fold_in(jax.random.fold_in(key, 6), dim), (parts,), jnp.float32, smallest / len(pieces), high / len(pieces))
        return jnp.repeat(jnp.exp(heights), dims[dim] // parts).reshape((-1,) + (1,) * (len(dims) - dim - 1))

    gain = one(*pieces[0])
    for cut in pieces[1:]:
        gain = gain * one(*cut)
    return gain


def scatter_about(key, shape, width, bound, cuts=(), held_as=jnp.bfloat16):
    drawn = width * jax.random.normal(key, shape, jnp.float32)
    if cuts:
        drawn = drawn * levels(key, shape, cuts, -0.22, 0.18)
    return jnp.clip(drawn, -bound, bound).astype(held_as)


def setup_inputs(seed: int = 0) -> dict:
    arg_keys = jax.random.split(jax.random.key(seed), 12)
    return {
        "features": scatter_about(arg_keys[0], (TOTAL, FEAT), 1.0, 6.0, ((0, 32),)),
        "w_one": scatter_about(arg_keys[1], (HID, FEAT), FEAT ** -0.5, 0.109375),
        "b_one": scatter_about(arg_keys[2], (HID,), 0.5, 3.0, (), jnp.float32),
        "w_two": scatter_about(arg_keys[3], (HID, ACTIONS * ATOMS), HID ** -0.5, 0.25),
        "b_two": draw_b_two(jax.random.fold_in(arg_keys[11], 71), 0),
        "action": with_ends(jax.random.randint(arg_keys[5], (TOTAL,), 0, ACTIONS), jax.random.fold_in(arg_keys[5], 1), 0, ACTIONS - 1).astype(jnp.int32),
        "target_probs": draw_target_probs(jax.random.fold_in(arg_keys[11], 71), 0),
        "next_action": with_ends(jax.random.randint(arg_keys[7], (TOTAL,), 0, ACTIONS), jax.random.fold_in(arg_keys[7], 1), 0, ACTIONS - 1).astype(jnp.int32),
        "lower_idx": with_ends(jax.random.randint(arg_keys[8], (TOTAL, ATOMS), 0, ATOMS - 1), jax.random.fold_in(arg_keys[8], 1), 0, (ATOMS - 1) - 1).astype(jnp.int32),
        "upper_frac": jnp.clip(1.0 * jax.random.uniform(arg_keys[9], (TOTAL, ATOMS), jnp.float32) ** levels(arg_keys[9], (TOTAL, ATOMS), ((0, 32),), -0.2, 0.2), 0.0, 1.0),
        "is_weight": jnp.clip(jnp.exp(math.log(1.0) - 2.3025851 * jax.random.uniform(arg_keys[10], (TOTAL,), jnp.float32) ** levels(arg_keys[10], (TOTAL,), ((0, 32),), -0.2, 0.2)), 0.1, 1.0),
    }


def forward_loss(features, w_one, b_one, w_two, b_two, action, target_probs, next_action, lower_idx, upper_frac, is_weight):
    row_count = features.shape[0]
    n_act = target_probs.shape[1]
    n_atom = target_probs.shape[2]
    pre_act = lax.dot_general(features, w_one, (((1,), (1,)), ((), ())), preferred_element_type=jnp.float32) + b_one
    hidden = jnp.maximum(pre_act, 0.0).astype(jnp.bfloat16)
    logits = (jnp.dot(hidden, w_two, preferred_element_type=jnp.float32) + b_two).reshape(row_count, n_act, n_atom)
    chosen = jnp.take_along_axis(logits, action.astype(jnp.int32)[:, None, None], axis=1)[:, 0, :]
    log_probs = jax.nn.log_softmax(chosen, axis=-1)
    next_probs = jnp.take_along_axis(target_probs, next_action.astype(jnp.int32)[:, None, None], axis=1)[:, 0, :]
    atom_ids = jnp.arange(n_atom, dtype=jnp.int32)
    mass_low = next_probs * (1.0 - upper_frac)
    mass_high = next_probs * upper_frac
    low_hot = lower_idx[:, :, None] == atom_ids[None, None, :]
    high_hot = (lower_idx[:, :, None] + 1) == atom_ids[None, None, :]
    projected = jnp.sum(jnp.where(low_hot, mass_low[:, :, None], 0.0) + jnp.where(high_hot, mass_high[:, :, None], 0.0), axis=1)
    cross_ent = -jnp.sum(projected * log_probs, axis=-1)
    grad_chosen = is_weight[:, None] * (jnp.exp(log_probs) * jnp.sum(projected, axis=-1, keepdims=True) - projected)
    act_hot = action[:, None] == jnp.arange(n_act, dtype=jnp.int32)[None, :]
    grad_logits = jnp.where(act_hot[:, :, None], grad_chosen[:, None, :], 0.0).reshape(row_count, n_act * n_atom).astype(jnp.bfloat16)
    grad_hidden = lax.dot_general(grad_logits, w_two, (((1,), (1,)), ((), ())), preferred_element_type=jnp.float32)
    grad_pre = jnp.where(pre_act > 0.0, grad_hidden, 0.0).astype(jnp.bfloat16)
    return hidden, grad_logits, grad_pre, cross_ent


def reference(features, w_one, b_one, w_two, b_two, action, target_probs, next_action, lower_idx, upper_frac, is_weight):
    def split_rows(array):
        return array.reshape((N_DP, ROWS) + array.shape[1:])

    blocks = tuple(split_rows(item) for item in (features, action, target_probs, next_action, lower_idx, upper_frac, is_weight))

    def step(carry, block):
        g_w1, g_b1, g_w2, g_b2, loss_sum, top = carry
        feat, act, probs, nxt, lower, frac, weight = block
        hidden, grad_logits, grad_pre, cross_ent = forward_loss(feat, w_one, b_one, w_two, b_two, act, probs, nxt, lower, frac, weight)
        g_w1 = g_w1 + lax.dot_general(grad_pre, feat, (((0,), (0,)), ((), ())), preferred_element_type=jnp.float32)
        g_b1 = g_b1 + jnp.sum(grad_pre.astype(jnp.float32), axis=0)
        g_w2 = g_w2 + lax.dot_general(hidden, grad_logits, (((0,), (0,)), ((), ())), preferred_element_type=jnp.float32)
        g_b2 = g_b2 + jnp.sum(grad_logits.astype(jnp.float32), axis=0)
        loss_sum = loss_sum + jnp.sum(weight * cross_ent)
        top = jnp.maximum(top, jnp.max(cross_ent))
        return (g_w1, g_b1, g_w2, g_b2, loss_sum, top), cross_ent

    start = (jnp.zeros(w_one.shape, jnp.float32), jnp.zeros(b_one.shape, jnp.float32),
             jnp.zeros(w_two.shape, jnp.float32), jnp.zeros(b_two.shape, jnp.float32),
             jnp.zeros((), jnp.float32), jnp.zeros((), jnp.float32))
    (g_w1, g_b1, g_w2, g_b2, loss_sum, top), losses = lax.scan(step, start, blocks)
    priorities = losses.reshape(-1) / jnp.maximum(top, 1.0)
    mean_loss = loss_sum / TOTAL
    return g_w1, g_b1, g_w2, g_b2, mean_loss, priorities
```

```python
import functools

import jax
import jax.numpy as jnp
from jax import lax
from jax.experimental import pallas as pl
from jax.experimental.pallas import tpu as pltpu
from jax.sharding import PartitionSpec as P

MESH = pl.DeviceIdType.MESH
F32 = jnp.float32
BF16 = jnp.bfloat16
VMEM_LIMIT = 60 * 1024 * 1024


def pad_up(value, step):
    return -(-value // step) * step


def dot(a, b, ca, cb):
    return lax.dot_general(a, b, (((ca,), (cb,)), ((), ())), preferred_element_type=F32)


def head_kernel(
    n_act, n_atom, slot,
    pre_ref, w2_ref, b2_ref, act_ref, tp_ref, nxt_ref, low_ref, frac_ref, wgt_ref,
    gp_ref, gw2_ref, gb1_ref, gb2_ref, ce_ref, acc_ref,
):
    step = pl.program_id(0)
    last = pl.num_programs(0) - 1
    pre = pre_ref[...]
    cols = pre.shape[1]
    hidden = jnp.maximum(pre, 0.0).astype(BF16)
    logits = dot(w2_ref[...], hidden, 1, 0) + b2_ref[...]
    act = act_ref[...]
    nxt = nxt_ref[...]
    chosen = jnp.zeros((slot, cols), F32)
    for a in range(n_act):
        chosen = jnp.where(act == a, logits[a * slot:(a + 1) * slot], chosen)
    atom = lax.broadcasted_iota(jnp.int32, (slot, cols), 0)
    real = atom < n_atom
    chosen = jnp.where(real, chosen, -jnp.inf)
    shifted = chosen - jnp.max(chosen, axis=0, keepdims=True)
    log_z = jnp.log(jnp.sum(jnp.exp(shifted), axis=0, keepdims=True))
    log_probs = jnp.where(real, shifted - log_z, 0.0)
    probs = jnp.where(real, jnp.exp(log_probs), 0.0)
    nprob = jnp.zeros((n_atom, cols), F32)
    for a in range(n_act):
        nprob = jnp.where(nxt == a, tp_ref[a], nprob)
    frac = frac_ref[...]
    mass_low = nprob * (1.0 - frac)
    mass_high = nprob * frac
    low = low_ref[...]
    proj = jnp.zeros((slot, cols), F32)
    for j in range(n_atom):
        dist = atom - low[j:j + 1]
        proj = proj + jnp.where(
            dist == 0, mass_low[j:j + 1], jnp.where(dist == 1, mass_high[j:j + 1], 0.0)
        )
    ce_ref[...] = -jnp.sum(proj * log_probs, axis=0, keepdims=True)
    grad = wgt_ref[...] * (probs * jnp.sum(proj, axis=0, keepdims=True) - proj)
    grad_logits = jnp.concatenate(
        [jnp.where(act == a, grad, 0.0).astype(BF16) for a in range(n_act)], axis=0
    )
    grad_hidden = dot(w2_ref[...], grad_logits, 0, 0)
    grad_pre = jnp.where(pre > 0.0, grad_hidden, 0.0).astype(BF16)
    gp_ref[...] = grad_pre
    ones = jnp.ones((8, cols), BF16)

    @pl.when(step == 0)
    def _():
        acc_ref[...] = jnp.zeros_like(acc_ref)
        gb1_ref[...] = jnp.zeros_like(gb1_ref)
        gb2_ref[...] = jnp.zeros_like(gb2_ref)

    acc_ref[...] += dot(grad_logits, hidden, 1, 1)
    gb1_ref[...] += dot(ones, grad_pre, 1, 1)
    gb2_ref[...] += dot(ones, grad_logits, 1, 1)

    @pl.when(step == last)
    def _():
        used = n_act * n_atom
        if gw2_ref.shape[0] > used:
            gw2_ref[used:, :] = jnp.zeros((gw2_ref.shape[0] - used, gw2_ref.shape[1]), F32)
        for a in range(n_act):
            gw2_ref[a * n_atom:(a + 1) * n_atom, :] = acc_ref[a * slot:a * slot + n_atom, :]


def head(pre, w2p, b2p, act, tp, nxt, low, frac, wgt, n_act, n_atom, slot):
    hid, rows = pre.shape
    tile = 256 if rows % 256 == 0 else rows
    wide = n_act * slot
    packed = pad_up(n_act * n_atom, 8)
    lanes = lambda height: pl.BlockSpec((height, tile), lambda i: (0, i))
    whole = lambda shape: pl.BlockSpec(shape, lambda i: (0,) * len(shape))
    return pl.pallas_call(
        functools.partial(head_kernel, n_act, n_atom, slot),
        grid=(rows // tile,),
        in_specs=[
            lanes(hid), whole((wide, hid)), whole((wide, 1)), lanes(1),
            pl.BlockSpec((n_act, n_atom, tile), lambda i: (0, 0, i)),
            lanes(1), lanes(n_atom), lanes(n_atom), lanes(1),
        ],
        out_specs=[lanes(hid), whole((packed, hid)), whole((8, hid)), whole((8, wide)), lanes(1)],
        out_shape=[
            jax.ShapeDtypeStruct((hid, rows), BF16),
            jax.ShapeDtypeStruct((packed, hid), F32),
            jax.ShapeDtypeStruct((8, hid), F32),
            jax.ShapeDtypeStruct((8, wide), F32),
            jax.ShapeDtypeStruct((1, rows), F32),
        ],
        scratch_shapes=[pltpu.VMEM((wide, hid), F32)],
        compiler_params=pltpu.CompilerParams(vmem_limit_bytes=VMEM_LIMIT),
        name="head",
    )(pre, w2p, b2p, act, tp, nxt, low, frac, wgt)


def plan(n_dev, used):
    bits = n_dev.bit_length() - 1
    unit = 8 * n_dev
    units = -(-used // unit)
    rest = list(range(1, bits))
    head_bits, tail_bits = rest[:3], rest[3:]
    orders = []
    for turn in range(max(1, len(head_bits))):
        orders.append([0] + head_bits[turn:] + head_bits[:turn] + tail_bits)
    light = len(orders) - 1
    names = [(s, o) for s in range(2) for o in range(len(orders))]
    give = [k for k in names if k[1] != light] + [k for k in names if k[1] == light]
    share = {k: 0 for k in names}
    for u in range(units):
        share[give[u % len(give)]] += 1
    parts, base = [], 0
    for k in names:
        if share[k]:
            parts.append((base, share[k] * unit, orders[k[1]]))
            base += share[k] * unit
    return parts, base


def chunk_of(rows):
    best = 8
    for c in range(8, 65, 8):
        if rows % c == 0:
            best = c
    return best


def sum_kernel(
    parts, bits, feat_ref, gp_ref, w2_ref, tail_ref, o1_ref, o2_ref, o3_ref,
    mine, heard, total, send_sem, recv_sem, out_sem,
):
    me = lax.axis_index("dp")
    n_feat = feat_ref.shape[0]
    n_w2 = w2_ref.shape[0]
    n_tail = tail_ref.shape[0]
    sections = ((0, n_feat, o1_ref), (n_feat, n_w2, o2_ref), (n_feat + n_w2, n_tail, o3_ref))

    def bit_of(b):
        return lax.rem(lax.div(me, 1 << b), 2)

    def partner(b):
        return me + (1 << b) - 2 * (1 << b) * bit_of(b)

    barrier = pltpu.get_barrier_semaphore()
    for b in range(bits):
        pl.semaphore_signal(barrier, inc=1, device_id=(partner(b),), device_id_type=MESH)
    pl.semaphore_wait(barrier, bits)

    def rows_at(offset, count):
        return pl.ds(pl.multiple_of(offset, 8), count)

    spans = []
    for base, length, order in parts:
        offs, off, here = [], base, length
        heard_at = base
        for b in order:
            half = here // 2
            keep = off + bit_of(b) * half
            away = off + (1 - bit_of(b)) * half
            offs.append((keep, away, half, heard_at))
            heard_at += half
            off, here = keep, half
        spans.append(offs)

    def scatter(p, i):
        keep, away, half, heard_at = spans[p][i]
        return pltpu.make_async_remote_copy(
            src_ref=mine.at[rows_at(away, half)],
            dst_ref=heard.at[pl.ds(heard_at, half)],
            send_sem=send_sem.at[p, i],
            recv_sem=recv_sem.at[p, i],
            device_id=(partner(parts[p][2][i]),),
            device_id_type=MESH,
        )

    def gather(p, i):
        keep, away, half, heard_at = spans[p][i]
        return pltpu.make_async_remote_copy(
            src_ref=total.at[rows_at(keep, half)],
            dst_ref=total.at[rows_at(keep, half)],
            send_sem=send_sem.at[p, bits + i],
            recv_sem=recv_sem.at[p, bits + i],
            device_id=(partner(parts[p][2][i]),),
            device_id_type=MESH,
        )

    for p, (base, length, order) in enumerate(parts):
        stop = base + length
        end = min(stop, n_feat)
        if end > base:
            full = (end - base) // 256

            @pl.loop(0, full)
            def _(k, base=base):
                at = rows_at(base + k * 256, 256)
                mine[at, :] = dot(feat_ref[at, :], gp_ref[...], 1, 1)

            left = base + full * 256
            if left < end:
                mine[left:end, :] = dot(feat_ref[left:end, :], gp_ref[...], 1, 1)
        for start, count, src in ((n_feat, n_w2, w2_ref), (n_feat + n_w2, n_tail, tail_ref)):
            lo, hi = max(base, start), min(stop, start + count)
            if hi > lo:
                mine[lo:hi, :] = src[lo - start:hi - start, :]
        scatter(p, 0).start()

    for i in range(bits):
        for p in range(len(parts)):
            scatter(p, i).wait_recv()
            keep, away, half, heard_at = spans[p][i]
            chunk = chunk_of(half)
            into = mine if i < bits - 1 else total

            @pl.loop(0, half // chunk)
            def _(k, keep=keep, heard_at=heard_at, chunk=chunk, into=into):
                at = rows_at(keep + k * chunk, chunk)
                into[at, :] = mine[at, :] + heard[rows_at(heard_at + k * chunk, chunk), :]

            if i < bits - 1:
                scatter(p, i + 1).start()
            else:
                gather(p, i).start()

    for i in range(bits - 1, -1, -1):
        for p in range(len(parts)):
            gather(p, i).wait_recv()
            if i > 0:
                gather(p, i - 1).start()

    copies = []
    for p, (base, length, order) in enumerate(parts):
        for s, (start, count, out) in enumerate(sections):
            lo, hi = max(base, start), min(base + length, start + count)
            if hi > lo:
                copy = pltpu.make_async_copy(
                    total.at[pl.ds(lo, hi - lo)], out.at[pl.ds(lo - start, hi - lo)], out_sem.at[p, s]
                )
                copy.start()
                copies.append(copy)
    for p in range(len(parts)):
        for i in range(bits):
            scatter(p, i).wait_send()
            gather(p, i).wait_send()
    for copy in copies:
        copy.wait()


def sum_over(n_dev, feat, gp, gw2, small):
    n_feat = feat.shape[0]
    hid = gp.shape[0]
    parts, height = plan(n_dev, n_feat + gw2.shape[0] + small.shape[0])
    room = height - n_feat - gw2.shape[0]
    small = jnp.pad(small, ((0, room - small.shape[0]), (0, 0)))
    bits = n_dev.bit_length() - 1
    whole = pl.BlockSpec(memory_space=pltpu.VMEM)
    anywhere = pl.BlockSpec(memory_space=pl.ANY)
    return pl.pallas_call(
        functools.partial(sum_kernel, parts, bits),
        in_specs=[whole] * 4,
        out_specs=[anywhere] * 3,
        out_shape=[
            jax.ShapeDtypeStruct((n_feat, hid), F32),
            jax.ShapeDtypeStruct(gw2.shape, F32),
            jax.ShapeDtypeStruct(small.shape, F32),
        ],
        scratch_shapes=[
            pltpu.VMEM((height, hid), F32),
            pltpu.VMEM((height, hid), F32),
            pltpu.VMEM((height, hid), F32),
            pltpu.SemaphoreType.DMA((len(parts), 2 * bits)),
            pltpu.SemaphoreType.DMA((len(parts), 2 * bits)),
            pltpu.SemaphoreType.DMA((len(parts), 3)),
        ],
        compiler_params=pltpu.CompilerParams(
            collective_id=0, has_side_effects=True, vmem_limit_bytes=VMEM_LIMIT
        ),
        name="sum_over_devices",
    )(feat, gp, gw2, small)


def on_device(
    n_dev, features, w_one, b_one, w_two, b_two, action, target_probs, next_action, lower_idx, upper_frac, is_weight,
):
    rows = features.shape[0]
    hid = w_one.shape[0]
    n_act, n_atom = target_probs.shape[1:]
    slot = pad_up(n_atom, 16)
    wide = n_act * slot
    feat = features.T
    pre = dot(w_one, features, 1, 1) + b_one[:, None]
    w2p = jnp.pad(w_two.T.reshape(n_act, n_atom, hid), ((0, 0), (0, slot - n_atom), (0, 0))).reshape(wide, hid)
    b2p = jnp.pad(b_two.reshape(n_act, n_atom), ((0, 0), (0, slot - n_atom))).reshape(wide, 1)
    gp, gw2, gb1, gb2, ce = head(
        pre, w2p, b2p, action[None, :], target_probs.transpose(1, 2, 0), next_action[None, :],
        lower_idx.T, upper_frac.T, is_weight[None, :], n_act, n_atom, slot,
    )
    ce = ce[0]
    tops = jnp.where(jnp.arange(hid) == lax.axis_index("dp"), jnp.max(ce), 0.0)
    loss = jnp.where(jnp.arange(hid) == 0, jnp.sum(is_weight * ce), 0.0)
    b2_rows = -(-wide // hid)
    b2_flat = jnp.pad(gb2[0], (0, b2_rows * hid - wide)).reshape(b2_rows, hid)
    small = jnp.concatenate([gb1[:1], tops[None], loss[None], b2_flat], axis=0)
    g1, g2, rest = sum_over(n_dev, feat, gp, gw2, small)
    top = jnp.max(jnp.where(jnp.arange(hid) < n_dev, rest[1], -jnp.inf))
    grad_b2 = rest[3:3 + b2_rows].reshape(-1)[:wide].reshape(n_act, slot)[:, :n_atom].reshape(-1)
    mean_loss = rest[2, 0] / (rows * n_dev)
    priorities = ce / jnp.maximum(top, 1.0)
    return g1.T, rest[0], g2[:n_act * n_atom].T, grad_b2, mean_loss, priorities


def solution(mesh):
    in_specs = (
        P("dp", None), P(), P(), P(), P(), P("dp"), P("dp", None, None), P("dp"),
        P("dp", None), P("dp", None), P("dp"),
    )
    out_specs = (P(), P(), P(), P(), P(), P("dp"))
    return jax.shard_map(
        functools.partial(on_device, mesh.shape["dp"]),
        mesh=mesh, in_specs=in_specs, out_specs=out_specs, check_vma=False,
    )
```

```python
import functools

import jax
import jax.numpy as jnp
from jax import lax
from jax.experimental import pallas as pl
from jax.experimental.pallas import tpu as pltpu
from jax.sharding import PartitionSpec as P

MESH = pl.DeviceIdType.MESH
F32 = jnp.float32
BF16 = jnp.bfloat16
HEAD_LIMIT = 60 * 1024 * 1024
SUM_LIMIT = 40 * 1024 * 1024
SETS = 3


def pad_up(value, step):
    return -(-value // step) * step


def dot(a, b, ca, cb):
    return lax.dot_general(a, b, (((ca,), (cb,)), ((), ())), preferred_element_type=F32)


def head_kernel(
    n_act, n_atom, slot,
    pre_ref, w2_ref, b2_ref, act_ref, tp_ref, nxt_ref, low_ref, frac_ref, wgt_ref,
    gp_ref, gw2_ref, gb1_ref, gb2_ref, ce_ref, acc_ref, w2p_ref, b2t_ref,
):
    step = pl.program_id(0)
    last = pl.num_programs(0) - 1

    @pl.when(step == 0)
    def _():
        w2p_ref[...] = jnp.zeros_like(w2p_ref)
        b2t_ref[...] = jnp.zeros_like(b2t_ref)
        b2t_ref[0:n_atom, 0:n_act] = b2_ref[...].T
        for a in range(n_act):
            w2p_ref[a * slot:a * slot + n_atom, :] = w2_ref[a * n_atom:(a + 1) * n_atom, :]

    pre = pre_ref[...]
    cols = pre.shape[1]
    hidden = jnp.maximum(pre, 0.0).astype(BF16)
    logits = dot(w2p_ref[...], hidden, 1, 0)
    bias = b2t_ref[...]
    act = act_ref[...]
    nxt = nxt_ref[...]
    chosen = jnp.zeros((slot, cols), F32)
    for a in range(n_act):
        chosen = jnp.where(act == a, logits[a * slot:(a + 1) * slot] + bias[:, a:a + 1], chosen)
    atom = lax.broadcasted_iota(jnp.int32, (slot, cols), 0)
    real = atom < n_atom
    chosen = jnp.where(real, chosen, -jnp.inf)
    shifted = chosen - jnp.max(chosen, axis=0, keepdims=True)
    log_z = jnp.log(jnp.sum(jnp.exp(shifted), axis=0, keepdims=True))
    log_probs = jnp.where(real, shifted - log_z, 0.0)
    probs = jnp.where(real, jnp.exp(log_probs), 0.0)
    nprob = jnp.zeros((n_atom, cols), F32)
    for a in range(n_act):
        nprob = jnp.where(nxt == a, tp_ref[a], nprob)
    frac = frac_ref[...]
    mass_low = nprob * (1.0 - frac)
    mass_high = nprob * frac
    low = low_ref[...]
    proj = jnp.zeros((slot, cols), F32)
    for j in range(n_atom):
        dist = atom - low[j:j + 1]
        proj = proj + jnp.where(
            dist == 0, mass_low[j:j + 1], jnp.where(dist == 1, mass_high[j:j + 1], 0.0)
        )
    ce_ref[...] = -jnp.sum(proj * log_probs, axis=0, keepdims=True)
    grad = wgt_ref[...] * (probs * jnp.sum(proj, axis=0, keepdims=True) - proj)
    grad_logits = jnp.concatenate(
        [jnp.where(act == a, grad, 0.0).astype(BF16) for a in range(n_act)], axis=0
    )
    grad_hidden = dot(w2p_ref[...], grad_logits, 0, 0)
    grad_pre = jnp.where(pre > 0.0, grad_hidden, 0.0).astype(BF16)
    gp_ref[...] = grad_pre
    ones = jnp.ones((8, cols), BF16)

    @pl.when(step == 0)
    def _():
        acc_ref[...] = jnp.zeros_like(acc_ref)
        gb1_ref[...] = jnp.zeros_like(gb1_ref)
        gb2_ref[...] = jnp.zeros_like(gb2_ref)

    acc_ref[...] += dot(grad_logits, hidden, 1, 1)
    gb1_ref[...] += dot(ones, grad_pre, 1, 1)
    gb2_ref[...] += dot(ones, grad_logits, 1, 1)

    @pl.when(step == last)
    def _():
        used = n_act * n_atom
        if gw2_ref.shape[0] > used:
            gw2_ref[used:, :] = jnp.zeros((gw2_ref.shape[0] - used, gw2_ref.shape[1]), F32)
        for a in range(n_act):
            gw2_ref[a * n_atom:(a + 1) * n_atom, :] = acc_ref[a * slot:a * slot + n_atom, :]


def head(pre, w2, b2, act, tp, nxt, low, frac, wgt, n_act, n_atom, slot):
    hid, rows = pre.shape
    tile = 256 if rows % 256 == 0 else rows
    wide = n_act * slot
    packed = pad_up(n_act * n_atom, 8)
    lanes = lambda height: pl.BlockSpec((height, tile), lambda i: (0, i))
    whole = lambda shape: pl.BlockSpec(shape, lambda i: (0,) * len(shape))
    return pl.pallas_call(
        functools.partial(head_kernel, n_act, n_atom, slot),
        grid=(rows // tile,),
        in_specs=[
            lanes(hid), whole(w2.shape), whole(b2.shape), lanes(1),
            pl.BlockSpec((n_act, n_atom, tile), lambda i: (0, 0, i)),
            lanes(1), lanes(n_atom), lanes(n_atom), lanes(1),
        ],
        out_specs=[lanes(hid), whole((packed, hid)), whole((8, hid)), whole((8, wide)), lanes(1)],
        out_shape=[
            jax.ShapeDtypeStruct((hid, rows), BF16),
            jax.ShapeDtypeStruct((packed, hid), F32),
            jax.ShapeDtypeStruct((8, hid), F32),
            jax.ShapeDtypeStruct((8, wide), F32),
            jax.ShapeDtypeStruct((1, rows), F32),
        ],
        scratch_shapes=[
            pltpu.VMEM((wide, hid), F32),
            pltpu.VMEM((wide, hid), BF16),
            pltpu.VMEM((slot, pad_up(n_act, 128)), F32),
        ],
        compiler_params=pltpu.CompilerParams(vmem_limit_bytes=HEAD_LIMIT),
        name="head",
    )(pre, w2, b2, act, tp, nxt, low, frac, wgt)


def plan(n_dev, used):
    bits = n_dev.bit_length() - 1
    unit = 8 * n_dev
    units = -(-used // unit)
    rest = list(range(1, bits))
    head_bits, tail_bits = rest[:3], rest[3:]
    orders = []
    for turn in range(max(1, len(head_bits))):
        orders.append([0] + head_bits[turn:] + head_bits[:turn] + tail_bits)
    light = len(orders) - 1
    names = [(s, o) for s in range(SETS) for o in range(len(orders))]
    give = [k for k in names if k[1] != light] + [k for k in names if k[1] == light]
    share = {k: 0 for k in names}
    for u in range(units):
        share[give[u % len(give)]] += 1
    parts, base = [], 0
    for k in names:
        if share[k]:
            parts.append((base, share[k] * unit, orders[k[1]]))
            base += share[k] * unit
    return parts, base


def chunk_of(rows):
    best = 8
    for c in range(8, 65, 8):
        if rows % c == 0:
            best = c
    return best


def sum_kernel(
    parts, bits, feat_hbm, gp_ref, w2_ref, gb1_ref, gb2_ref, ce_ref, wgt_ref,
    o1_ref, o2_ref, o3_ref, prio_ref,
    mine, heard, total, feat_ref, send_sem, recv_sem, out_sem, in_sem,
):
    me = lax.axis_index("dp")
    n_feat = feat_ref.shape[0]
    n_w2 = w2_ref.shape[0]
    n_tail = o3_ref.shape[0]
    hid = gp_ref.shape[0]
    tail_at = n_feat + n_w2

    loads = []
    for p, (base, length, order) in enumerate(parts):
        end = min(base + length, n_feat)
        if end > base:
            at = pl.ds(base, end - base)
            loads.append(pltpu.make_async_copy(feat_hbm.at[at], feat_ref.at[at], in_sem.at[p]))
            loads[-1].start()
        else:
            loads.append(None)
    sections = ((0, n_feat, o1_ref), (n_feat, n_w2, o2_ref), (n_feat + n_w2, n_tail, o3_ref))

    def bit_of(b):
        return lax.rem(lax.div(me, 1 << b), 2)

    def partner(b):
        return me + (1 << b) - 2 * (1 << b) * bit_of(b)

    barrier = pltpu.get_barrier_semaphore()
    for b in range(bits):
        pl.semaphore_signal(barrier, inc=1, device_id=(partner(b),), device_id_type=MESH)
    pl.semaphore_wait(barrier, bits)

    def rows_at(offset, count):
        return pl.ds(pl.multiple_of(offset, 8), count)

    spans = []
    for base, length, order in parts:
        offs, off, here = [], base, length
        heard_at = base
        for b in order:
            half = here // 2
            keep = off + bit_of(b) * half
            away = off + (1 - bit_of(b)) * half
            offs.append((keep, away, half, heard_at))
            heard_at += half
            off, here = keep, half
        spans.append(offs)

    def scatter(p, i):
        keep, away, half, heard_at = spans[p][i]
        return pltpu.make_async_remote_copy(
            src_ref=mine.at[rows_at(away, half)],
            dst_ref=heard.at[pl.ds(heard_at, half)],
            send_sem=send_sem.at[p, i],
            recv_sem=recv_sem.at[p, i],
            device_id=(partner(parts[p][2][i]),),
            device_id_type=MESH,
        )

    def gather(p, i):
        keep, away, half, heard_at = spans[p][i]
        return pltpu.make_async_remote_copy(
            src_ref=total.at[rows_at(keep, half)],
            dst_ref=total.at[rows_at(keep, half)],
            send_sem=send_sem.at[p, bits + i],
            recv_sem=recv_sem.at[p, bits + i],
            device_id=(partner(parts[p][2][i]),),
            device_id_type=MESH,
        )

    for p, (base, length, order) in enumerate(parts):
        stop = base + length
        end = min(stop, n_feat)
        if end > base:
            loads[p].wait()
            full = (end - base) // 256

            @pl.loop(0, full)
            def _(k, base=base):
                at = rows_at(base + k * 256, 256)
                mine[at, :] = dot(feat_ref[at, :], gp_ref[...], 1, 1)

            left = base + full * 256
            if left < end:
                mine[left:end, :] = dot(feat_ref[left:end, :], gp_ref[...], 1, 1)
        lo, hi = max(base, n_feat), min(stop, tail_at)
        if hi > lo:
            mine[lo:hi, :] = w2_ref[lo - n_feat:hi - n_feat, :]
        lo, hi = max(base, tail_at), stop
        if hi > lo:
            mine[lo:hi, :] = jnp.zeros((hi - lo, hid), F32)
            ce = ce_ref[...]
            lane = lax.broadcasted_iota(jnp.int32, (1, hid), 1)
            rows = [
                gb1_ref[0:1, :],
                jnp.where(lane == me, jnp.max(ce, axis=1, keepdims=True), 0.0),
                jnp.where(lane == 0, jnp.sum(ce * wgt_ref[...], axis=1, keepdims=True), 0.0),
            ]
            for at in range(0, gb2_ref.shape[1], hid):
                rows.append(gb2_ref[0:1, at:min(at + hid, gb2_ref.shape[1])])
            for r, row in enumerate(rows):
                if lo <= tail_at + r < hi:
                    mine[tail_at + r:tail_at + r + 1, 0:row.shape[1]] = row
        scatter(p, 0).start()

    for i in range(bits):
        for p in range(len(parts)):
            scatter(p, i).wait_recv()
            keep, away, half, heard_at = spans[p][i]
            chunk = chunk_of(half)
            into = mine if i < bits - 1 else total

            @pl.loop(0, half // chunk)
            def _(k, keep=keep, heard_at=heard_at, chunk=chunk, into=into):
                at = rows_at(keep + k * chunk, chunk)
                into[at, :] = mine[at, :] + heard[rows_at(heard_at + k * chunk, chunk), :]

            if i < bits - 1:
                scatter(p, i + 1).start()
            else:
                gather(p, i).start()

    copies = []
    for i in range(bits - 1, -1, -1):
        for p, (base, length, order) in enumerate(parts):
            gather(p, i).wait_recv()
            if i > 0:
                gather(p, i - 1).start()
                continue
            for s, (start, count, out) in enumerate(sections):
                lo, hi = max(base, start), min(base + length, start + count)
                if hi > lo:
                    copies.append(pltpu.make_async_copy(
                        total.at[pl.ds(lo, hi - lo)], out.at[pl.ds(lo - start, hi - lo)], out_sem.at[p, s]
                    ))
                    copies[-1].start()

    lane = lax.broadcasted_iota(jnp.int32, (1, hid), 1)
    tops = jnp.where(lane < (1 << bits), total[tail_at + 1:tail_at + 2, :], -jnp.inf)
    prio_ref[...] = ce_ref[...] / jnp.maximum(jnp.max(tops, axis=1, keepdims=True), 1.0)
    for p in range(len(parts)):
        for i in range(bits):
            scatter(p, i).wait_send()
            gather(p, i).wait_send()
    for copy in copies:
        copy.wait()


def sum_over(n_dev, feat, gp, gw2, gb1, gb2, ce, wgt):
    n_feat = feat.shape[0]
    hid = gp.shape[0]
    parts, height = plan(n_dev, n_feat + gw2.shape[0] + 3 - (-gb2.shape[1] // hid))
    room = height - n_feat - gw2.shape[0]
    bits = n_dev.bit_length() - 1
    whole = pl.BlockSpec(memory_space=pltpu.VMEM)
    anywhere = pl.BlockSpec(memory_space=pl.ANY)
    return pl.pallas_call(
        functools.partial(sum_kernel, parts, bits),
        in_specs=[anywhere] + [whole] * 6,
        out_specs=[anywhere] * 3 + [whole],
        out_shape=[
            jax.ShapeDtypeStruct((n_feat, hid), F32),
            jax.ShapeDtypeStruct(gw2.shape, F32),
            jax.ShapeDtypeStruct((room, hid), F32),
            jax.ShapeDtypeStruct(ce.shape, F32),
        ],
        scratch_shapes=[
            pltpu.VMEM((height, hid), F32),
            pltpu.VMEM((height, hid), F32),
            pltpu.VMEM((height, hid), F32),
            pltpu.VMEM(feat.shape, feat.dtype),
            pltpu.SemaphoreType.DMA((len(parts), 2 * bits)),
            pltpu.SemaphoreType.DMA((len(parts), 2 * bits)),
            pltpu.SemaphoreType.DMA((len(parts), 3)),
            pltpu.SemaphoreType.DMA((len(parts),)),
        ],
        compiler_params=pltpu.CompilerParams(
            collective_id=0, has_side_effects=True, vmem_limit_bytes=SUM_LIMIT
        ),
        name="sum_over_devices",
    )(feat, gp, gw2, gb1, gb2, ce, wgt)


def on_device(
    n_dev, features, w_one, b_one, w_two, b_two, action, target_probs, next_action, lower_idx, upper_frac, is_weight,
):
    rows = features.shape[0]
    hid = w_one.shape[0]
    n_act, n_atom = target_probs.shape[1:]
    slot = pad_up(n_atom, 16)
    wide = n_act * slot
    feat = features.T
    pre = dot(w_one, features, 1, 1) + b_one[:, None]
    gp, gw2, gb1, gb2, ce = head(
        pre, w_two.T, b_two.reshape(n_act, n_atom), action[None, :], target_probs.transpose(1, 2, 0),
        next_action[None, :], lower_idx.T, upper_frac.T, is_weight[None, :], n_act, n_atom, slot,
    )
    g1, g2, rest, priorities = sum_over(n_dev, feat, gp, gw2, gb1, gb2, ce, is_weight[None, :])
    b2_rows = -(-wide // hid)
    grad_b2 = rest[3:3 + b2_rows].reshape(-1)[:wide].reshape(n_act, slot)[:, :n_atom].reshape(-1)
    mean_loss = rest[2, 0] / (rows * n_dev)
    return g1.T, rest[0], g2[:n_act * n_atom].T, grad_b2, mean_loss, priorities[0]


def solution(mesh):
    in_specs = (
        P("dp", None), P(), P(), P(), P(), P("dp"), P("dp", None, None), P("dp"),
        P("dp", None), P("dp", None), P("dp"),
    )
    out_specs = (P(), P(), P(), P(), P(), P("dp"))
    return jax.shard_map(
        functools.partial(on_device, mesh.shape["dp"]),
        mesh=mesh, in_specs=in_specs, out_specs=out_specs, check_vma=False,
    )
```
